32 devices in a mesh: dp: 8 (over y, x, core), tensor: 4 (over z).
Axes of the slice: x: 2, y: 2, z: 4, core: 2. Of those that a mesh axis runs over, the one named last changes fastest.
Arguments:
- activations: bfloat16 [8, 1024, 1536], P('dp', 'tensor'), may hold values from -6 to 6
- lengths: int32 [8], P('dp'), may hold values from 256 to 1024, as said below
- attn_gain: bfloat16 [1536], P('dp'), may hold values from 0.5 to 1.5
- w_query: bfloat16 [1536, 1536], P('dp', 'tensor'), may hold values from -0.15625 to 0.15625
- w_key: bfloat16 [1536, 768], P('dp', 'tensor'), may hold values from -0.15625 to 0.15625
- w_value: bfloat16 [1536, 768], P('dp', 'tensor'), may hold values from -0.15625 to 0.15625
- w_out: bfloat16 [1536, 1536], P('tensor', 'dp'), may hold values from -3 to 3
- mlp_gain: bfloat16 [1536], P('dp'), may hold values from 0.5 to 1.5
- w_gate: bfloat16 [1536, 4096], P('dp', 'tensor'), may hold values from -0.15625 to 0.15625
- w_up: bfloat16 [1536, 4096], P('dp', 'tensor'), may hold values from -0.15625 to 0.15625
- w_down: bfloat16 [4096, 1536], P('tensor', 'dp'), may hold values from -0.09375 to 0.09375
- cotangent: bfloat16 [8, 1024, 1536], P('dp', 'tensor'), may hold values from -6 to 6
Outputs:
- out_acts: float32 [8, 1024, 1536], P('dp', 'tensor')
- grad_acts: float32 [8, 1024, 1536], P('dp', 'tensor')
- grad_attn_gain: float32 [1536], P('dp')
- grad_query: float32 [1536, 1536], P('dp', 'tensor')
- grad_key: float32 [1536, 768], P('dp', 'tensor')
- grad_value: float32 [1536, 768], P('dp', 'tensor')
- grad_out: float32 [1536, 1536], P('tensor', 'dp')
- grad_mlp_gain: float32 [1536], P('dp')
- grad_gate: float32 [1536, 4096], P('dp', 'tensor')
- grad_up: float32 [1536, 4096], P('dp', 'tensor')
- grad_down: float32 [4096, 1536], P('tensor', 'dp')
The draws below stay inside these ranges and needn't reach their ends.
Inputs may be any that keep to these rules, and one draw needn't show every extreme that they name: `lengths`: valid slots of each sequence; in every draw one sequence is full (1024) and one has exactly 256.
All inputs are finite; a program needn't handle non-finite values.
Results may differ from the reference program's by a relative error of at most 0.017.
Values may be sent and summed in bfloat16 or wider, within the bound.
A program may use at most 192 MiB of HBM per device.

```python
import math
import jax
import jax.numpy as jnp
from jax import lax

D = 1536
HEADS = 16
KV_HEADS = 8
HEAD_DIM = 96
FF = 4096
SEQ = 1024
SEQS = 8


def draw_lengths(key, part):
    shortest = SEQ // 4
    drawn = jax.random.randint(jax.random.fold_in(key, 11), (SEQS,), shortest, SEQ + 1)
    order = jax.random.permutation(jax.random.fold_in(key, 12), SEQS)
    drawn = drawn.at[order[0]].set(SEQ)
    drawn = drawn.at[order[1]].set(shortest)
    return drawn.astype(jnp.int32)


def spiked(array, stream_key, source, target, shards_of, factor):
    def block_of(axis_at):
        return (jnp.arange(array.shape[axis_at]) // (array.shape[axis_at] // shards_of)).reshape((-1,) + (1,) * (array.ndim - 1 - axis_at))

    first = jax.random.permutation(stream_key, shards_of)[block_of(target)]
    other_side = (block_of(target) + shards_of // 2) % shards_of
    return jnp.where((block_of(source) == first) | (block_of(source) == other_side), factor * array, array)


def steps_of(rng, extent, cuts, low, top_value):
    gain, own = 1.0, jax.random.fold_in(rng, 6)
    for dim, shards_of in cuts:
        draws = jnp.exp(jax.random.uniform(jax.random.fold_in(own, dim), (shards_of,), jnp.float32, low / len(cuts), top_value / len(cuts)))
        gain = gain * jnp.repeat(draws, extent[dim] // shards_of).reshape([-1 if axis == dim else 1 for axis in range(len(extent))])
    return gain


def gaussian(own_key, extent, scale, reach, split=(), kind=jnp.bfloat16):
    values = scale * jax.random.normal(own_key, extent, jnp.float32)
    if split:
        values = values * steps_of(own_key, extent, split, -0.22, 0.18)
    return jnp.clip(values, -reach, reach).astype(kind)


def heavy_noise(stream_key, dims, deviation, limit, pieces, heavy, kind=jnp.bfloat16):
    values = deviation * jax.random.normal(stream_key, dims, jnp.float32)
    if pieces:
        values = values * steps_of(stream_key, dims, pieces, -0.22, 0.18)
    return jnp.clip(spiked(values, jax.random.fold_in(stream_key, 3), *heavy), -limit, limit).astype(kind)


def setup_inputs(seed: int = 0) -> dict:
    arg_keys = jax.random.split(jax.random.key(seed), 13)
    return {
        "activations": heavy_noise(arg_keys[0], (SEQS, SEQ, D), 1.0, 6.0, ((0, 8), (1, 4)), (0, 2, 8, 2.0)),
        "lengths": draw_lengths(jax.random.fold_in(arg_keys[12], 71), 0),
        "attn_gain": jnp.clip(1.0 + 0.1 * jax.random.normal(arg_keys[2], (D,), jnp.float32), 0.5, 1.5).astype(jnp.bfloat16),
        "w_query": gaussian(arg_keys[3], (D, D), D ** -0.5, 0.15625, ((0, 8), (1, 4))),
        "w_key": gaussian(arg_keys[4], (D, KV_HEADS * HEAD_DIM), D ** -0.5, 0.15625, ((0, 8), (1, 4))),
        "w_value": gaussian(arg_keys[5], (D, KV_HEADS * HEAD_DIM), D ** -0.5, 0.15625, ((0, 8), (1, 4))),
        "w_out": gaussian(arg_keys[6], (D, D), (max(D // 384, 4)) ** -0.5, 3.0, ((0, 4), (1, 8))),
        "mlp_gain": jnp.clip(1.0 + 0.1 * jax.random.normal(arg_keys[7], (D,), jnp.float32), 0.5, 1.5).astype(jnp.bfloat16),
        "w_gate": gaussian(arg_keys[8], (D, FF), D ** -0.5, 0.15625, ((0, 8), (1, 4))),
        "w_up": gaussian(arg_keys[9], (D, FF), D ** -0.5, 0.15625, ((0, 8), (1, 4))),
        "w_down": gaussian(arg_keys[10], (FF, D), FF ** -0.5, 0.09375, ((0, 4), (1, 8))),
        "cotangent": heavy_noise(arg_keys[11], (SEQS, SEQ, D), 1.0, 6.0, ((0, 8), (1, 4)), (0, 2, 8, 2.0)),
    }


@jax.custom_vjp
def low(v):
    return lax.optimization_barrier(v.astype(jnp.bfloat16)).astype(jnp.float32)

@jax.custom_vjp
def low_back(v):
    return v

def low_keep(v):
    return (low(v), None)

def low_pass(kept, grad):
    return (grad,)

def back_keep(v):
    return (v, None)

def back_low(kept, grad):
    return (low(grad),)
low.defvjp(low_keep, low_pass)
low_back.defvjp(back_keep, back_low)
EPS = 1e-05
THETA = 100000.0
NEG = -1e+30

def matmul(left, right):
    return jnp.dot(left, right, precision=lax.Precision.HIGHEST, preferred_element_type=jnp.float32)

def rope_tables(count, width):
    half = width // 2
    freqs = THETA ** (-jnp.arange(half, dtype=jnp.float32) * (2.0 / width))
    angles = jnp.arange(count, dtype=jnp.float32)[:, None] * freqs[None, :]
    return (jnp.cos(angles), jnp.sin(angles))

def rotate(vectors, cosines, sines):
    half = vectors.shape[-1] // 2
    first = vectors[..., :half]
    second = vectors[..., half:]
    cos_b = cosines[:, None, :]
    sin_b = sines[:, None, :]
    return jnp.concatenate([first * cos_b - second * sin_b, second * cos_b + first * sin_b], axis=-1)

def layer(tokens, length, attn_gain, w_query, w_key, w_value, w_out, mlp_gain, w_gate, w_up, w_down):
    groups = HEADS // KV_HEADS
    scale = 1.0 / math.sqrt(HEAD_DIM)
    positions = jnp.arange(SEQ)
    valid = positions < length
    cosines, sines = rope_tables(SEQ, HEAD_DIM)
    inv_first = lax.rsqrt(lax.optimization_barrier(jnp.mean(tokens * tokens, axis=1, keepdims=True)) + EPS)
    normed = low(tokens * inv_first * attn_gain)
    queries = low(rotate(low_back(matmul(normed, w_query)).reshape(SEQ, HEADS, HEAD_DIM), cosines, sines))
    keys = low(rotate(low_back(matmul(normed, w_key)).reshape(SEQ, KV_HEADS, HEAD_DIM), cosines, sines))
    values = low(low_back(matmul(normed, w_value))).reshape(SEQ, KV_HEADS, HEAD_DIM)
    block = min(512, SEQ)
    starts = jnp.arange(SEQ // block) * block
    query_blocks = queries.reshape(SEQ // block, block, KV_HEADS, groups, HEAD_DIM)

    def attend(item):
        query_block, start = item
        scores = jnp.einsum('qcgd,kcd->cgqk', query_block, keys, precision=lax.Precision.HIGHEST) * scale
        scores = low_back(scores)
        rows = start + jnp.arange(block)
        allowed = (positions[None, :] <= rows[:, None]) & valid[None, :]
        scores = jnp.where(allowed, scores, NEG)
        peak = lax.optimization_barrier(jnp.max(scores, axis=3, keepdims=True))
        log_sum = peak + jnp.log(lax.optimization_barrier(jnp.sum(jnp.exp(scores - peak), axis=3, keepdims=True)))
        probs = jnp.exp(scores - log_sum)
        return jnp.einsum('cgqk,kcd->qcgd', low(probs), values, precision=lax.Precision.HIGHEST)
    mixed = lax.map(jax.checkpoint(attend), (query_blocks, starts))
    attended = low(low_back(mixed.reshape(SEQ, HEADS * HEAD_DIM)))
    branch = low_back(matmul(attended, w_out))
    middle = tokens + branch
    inv_second = lax.rsqrt(lax.optimization_barrier(jnp.mean(middle * middle, axis=1, keepdims=True)) + EPS)
    normed_two = low(middle * inv_second * mlp_gain)
    gate = low_back(matmul(normed_two, w_gate))
    up_part = low_back(matmul(normed_two, w_up))
    hidden = low(jax.nn.silu(gate) * up_part)
    result = middle + low_back(matmul(hidden, w_down))
    return jnp.where(valid[:, None], result, 0.0)

def reference(activations, lengths, attn_gain, w_query, w_key, w_value, w_out, mlp_gain, w_gate, w_up, w_down, cotangent):

    def forward(tokens, gain_one, query_w, key_w, value_w, out_w, gain_two, gate_w, up_w, down_w):

        def one(carry, item):
            seq_tokens, length = item
            result = jax.checkpoint(layer)(seq_tokens, length, gain_one, query_w, key_w, value_w, out_w, gain_two, gate_w, up_w, down_w)
            return (carry, result)
        _, outputs = lax.scan(one, jnp.zeros((), jnp.float32), (tokens, lengths))
        return outputs
    outputs, pull = jax.vjp(forward, activations.astype(jnp.float32), attn_gain.astype(jnp.float32), w_query.astype(jnp.float32), w_key.astype(jnp.float32), w_value.astype(jnp.float32), w_out.astype(jnp.float32), mlp_gain.astype(jnp.float32), w_gate.astype(jnp.float32), w_up.astype(jnp.float32), w_down.astype(jnp.float32))
    grads = pull(cotangent.astype(jnp.float32))
    return (outputs, grads[0], grads[1], grads[2], grads[3], grads[4], grads[5], grads[6], grads[7], grads[8], grads[9])
```

```python
import math

import functools

import jax
import jax.numpy as jnp
from jax import lax
from jax.experimental import pallas as pl
from jax.experimental.pallas import tpu as pltpu
from jax.sharding import PartitionSpec as P

MESH = pl.DeviceIdType.MESH
CHUNKS = 4
BF = jnp.bfloat16
F32 = jnp.float32


def greet_line(me, n):
    barrier = pltpu.get_barrier_semaphore()
    for step in (-1, 1):
        there = (me + step >= 0) & (me + step < n)

        @pl.when(there)
        def _():
            pl.semaphore_signal(
                barrier, inc=1, device_id={"tensor": me + step}, device_id_type=MESH
            )

    near = jnp.where(me > 0, 1, 0) + jnp.where(me < n - 1, 1, 0)
    pl.semaphore_wait(barrier, near)


def block(index, piece, rows):
    size = rows // CHUNKS
    return pl.ds(pl.multiple_of(index * rows + piece * size, size), size)


class Gather:
    def __init__(self, me, n, own, out, send, recv):
        self.me, self.n, self.own, self.out = me, n, own, out
        self.send, self.recv = send, recv
        self.rows = own.shape[0]

    def copy(self, way, index, piece, first=False):
        there = self.out.at[block(index, piece, self.rows)]
        return pltpu.make_async_remote_copy(
            src_ref=self.own.at[block(0, piece, self.rows)] if first else there,
            dst_ref=there,
            send_sem=self.send.at[(way + 1) // 2, index, piece],
            recv_sem=self.recv.at[index, piece],
            device_id={"tensor": self.me + way},
            device_id_type=MESH,
        )

    def goes(self, way):
        return (self.me + way >= 0) & (self.me + way < self.n)

    def pass_on(self, way, index, piece):
        @pl.when((index == self.me) & self.goes(way))
        def _():
            self.copy(way, index, piece, True).start()

        @pl.when(((self.me - index) * way > 0) & (index >= 0) & (index < self.n))
        def _():
            self.copy(way, index, piece).wait_recv()

            @pl.when(self.goes(way))
            def _():
                self.copy(way, index, piece).start()

    def close(self, piece):
        for index in range(self.n):
            for way in (1, -1):

                @pl.when((index == self.me) & self.goes(way))
                def _():
                    self.copy(way, index, piece, True).wait_send()

                @pl.when(((self.me - index) * way > 0) & self.goes(way))
                def _():
                    self.copy(way, index, piece).wait_send()


class Scatter:
    def __init__(self, me, n, part, inbox, send, recv):
        self.me, self.n, self.part, self.inbox = me, n, part, inbox
        self.send, self.recv = send, recv
        self.rows = part.shape[0] // n

    def copy(self, way, owner, piece):
        there = block(owner, piece, self.rows)
        return pltpu.make_async_remote_copy(
            src_ref=self.part.at[there],
            dst_ref=self.inbox.at[(way + 1) // 2, there],
            send_sem=self.send.at[owner, piece],
            recv_sem=self.recv.at[(way + 1) // 2, owner, piece],
            device_id={"tensor": self.me + way},
            device_id_type=MESH,
        )

    def comes(self, way):
        return (self.me - way >= 0) & (self.me - way < self.n)

    def pass_on(self, way, owner, piece):
        @pl.when((owner - self.me) * way > 0)
        def _():
            @pl.when(self.comes(way))
            def _():
                self.copy(way, owner, piece).wait_recv()
                here = block(owner, piece, self.rows)
                self.part[here] = (
                    self.part[here].astype(F32) + self.inbox[(way + 1) // 2, here].astype(F32)
                ).astype(BF)

            self.copy(way, owner, piece).start()

    def finish(self, piece, total):
        here = block(self.me, piece, self.rows)
        there = block(0, piece, self.rows)
        total[there] = self.part[here].astype(F32)
        for way in (1, -1):

            @pl.when(self.comes(way))
            def _():
                self.copy(way, self.me, piece).wait_recv()
                total[there] += self.inbox[(way + 1) // 2, here].astype(F32)

    def close(self, piece):
        for owner in range(self.n):
            for way in (1, -1):

                @pl.when((owner - self.me) * way > 0)
                def _():
                    self.copy(way, owner, piece).wait_send()


def pieces(step):
    lax.fori_loop(0, CHUNKS, lambda piece, carry: (step(piece), carry)[1], 0)


LAG = 1


def both_ways(me, n, steps, act):
    near = jnp.where(2 * me < n, 1, -1)
    count = steps * CHUNKS

    def body(index, carry):
        for way, late in ((near, 0), (-near, LAG)):
            at = index - late

            @pl.when((at >= 0) & (at < count))
            def _():
                act(way, at // CHUNKS, at % CHUNKS)

        return carry

    lax.fori_loop(0, count + LAG, body, 0)


def exchange_kernel(n, gathers, scatters, *refs):
    refs = list(refs)
    own = refs.pop(0) if gathers else None
    source = refs.pop(0) if scatters else None
    out = refs.pop(0) if gathers else None
    total = refs.pop(0) if scatters else None
    me = lax.axis_index("tensor")
    gather = scatter = None
    if gathers:
        local, send, recv = refs[:3]
        refs = refs[3:]
        gather = Gather(me, n, own, out, send, recv)
    if scatters:
        part, inbox, load, send, recv = refs
        scatter = Scatter(me, n, part, inbox, send, recv)
        fetch = pltpu.make_async_copy(source, part, load)
        fetch.start()
    greet_line(me, n)
    if gathers:
        keep = pltpu.make_async_copy(own, out.at[pl.ds(me * own.shape[0], own.shape[0])], local)
        keep.start()
    if scatters:
        fetch.wait()

    def act(way, step, piece):
        if scatters:
            index = jnp.where(way > 0, n - 1 - step, step)

            @pl.when(step < n - 1)
            def _():
                scatter.pass_on(way, index, piece)

        if gathers:
            gather.pass_on(way, me - way * step, piece)

    both_ways(me, n, n if gathers else n - 1, act)
    if scatters:
        pieces(lambda piece: scatter.finish(piece, total))
        pieces(scatter.close)
    if gathers:
        pieces(gather.close)
        keep.wait()


def exchange(number, own=None, part=None):
    n = lax.axis_size("tensor")
    gathers, scatters = own is not None, part is not None
    anywhere = pl.BlockSpec(memory_space=pl.ANY)
    operands, in_specs, out_shape, out_specs, scratch = [], [], [], [], []
    if gathers:
        operands.append(own)
        in_specs.append(anywhere)
        out_shape.append(jax.ShapeDtypeStruct((n * own.shape[0], own.shape[1]), own.dtype))
        out_specs.append(anywhere)
        scratch += [
            pltpu.SemaphoreType.DMA,
            pltpu.SemaphoreType.DMA((2, n, CHUNKS)),
            pltpu.SemaphoreType.DMA((n, CHUNKS)),
        ]
    if scatters:
        operands.append(part)
        in_specs.append(anywhere)
        out_shape.append(jax.ShapeDtypeStruct((part.shape[0] // n, part.shape[1]), F32))
        out_specs.append(pl.BlockSpec(memory_space=pltpu.VMEM))
        scratch += [
            pltpu.VMEM(part.shape, BF),
            pltpu.VMEM((2,) + part.shape, BF),
            pltpu.SemaphoreType.DMA,
            pltpu.SemaphoreType.DMA((n, CHUNKS)),
            pltpu.SemaphoreType.DMA((2, n, CHUNKS)),
        ]
    return pl.pallas_call(
        functools.partial(exchange_kernel, n, gathers, scatters),
        out_shape=out_shape,
        in_specs=in_specs,
        out_specs=out_specs,
        scratch_shapes=scratch,
        compiler_params=pltpu.CompilerParams(collective_id=number, has_side_effects=True),
        name=f"exchange_{number}",
    )(*operands)


def greet_peers(axes):
    barrier = pltpu.get_barrier_semaphore()
    for axis in axes:
        me, n = lax.axis_index(axis), lax.axis_size(axis)

        def greet(step, carry):
            pl.semaphore_signal(
                barrier, inc=1, device_id={axis: lax.rem(me + step, n)}, device_id_type=MESH
            )
            return carry

        lax.fori_loop(1, n, greet, 0)
    pl.semaphore_wait(barrier, sum(lax.axis_size(axis) - 1 for axis in axes))


def to_peers(axis, source, inbox, send, recv):
    me, n = lax.axis_index(axis), lax.axis_size(axis)

    def copy(step, back):
        peer = lax.rem(me + step, n)
        slot = lax.rem(me + n - step, n) if back else me
        return pltpu.make_async_remote_copy(
            src_ref=source(peer),
            dst_ref=inbox.at[slot],
            send_sem=send.at[step],
            recv_sem=recv.at[slot],
            device_id={axis: peer},
            device_id_type=MESH,
        )

    def over(act):
        lax.fori_loop(1, n, lambda step, carry: (act(step), carry)[1], 0)

    over(lambda step: copy(step, False).start())
    over(lambda step: copy(step, True).wait_recv())
    return lambda: over(lambda step: copy(step, False).wait_send())


def gain_gather_kernel(own, out, send, recv):
    greet_peers(("dp",))
    out[lax.axis_index("dp")] = own[...]
    to_peers("dp", lambda peer: own, out, send, recv)()


def gain_gather(number, own):
    n = lax.axis_size("dp")
    inside = pl.BlockSpec(memory_space=pltpu.VMEM)
    whole = pl.pallas_call(
        gain_gather_kernel,
        out_shape=jax.ShapeDtypeStruct((n,) + own.shape, F32),
        in_specs=[inside],
        out_specs=inside,
        scratch_shapes=[pltpu.SemaphoreType.DMA((n,))] * 2,
        compiler_params=pltpu.CompilerParams(collective_id=number, has_side_effects=True),
        name="gain_gather",
    )(own)
    return whole.transpose(1, 0, 2).reshape(own.shape[0], -1)


def gain_sum_kernel(part, out, first, second, half, *sems):
    greet_peers(("dp", "tensor"))
    me, line = lax.axis_index("dp"), lax.axis_index("tensor")
    first[me] = part[me]
    done = to_peers("dp", lambda peer: part.at[peer], first, sems[0], sems[1])
    half[...] = jnp.sum(first[...], axis=0)
    second[line] = half[...]
    done_too = to_peers("tensor", lambda peer: half, second, sems[2], sems[3])
    out[...] = jnp.sum(second[...], axis=0)
    done()
    done_too()


def gain_sum(number, part):
    n, m = lax.axis_size("dp"), lax.axis_size("tensor")
    kinds = part.shape[0]
    cut = part.reshape(kinds, n, -1).transpose(1, 0, 2)
    one = cut.shape[1:]
    inside = pl.BlockSpec(memory_space=pltpu.VMEM)
    return pl.pallas_call(
        gain_sum_kernel,
        out_shape=jax.ShapeDtypeStruct(one, F32),
        in_specs=[inside],
        out_specs=inside,
        scratch_shapes=[
            pltpu.VMEM((n,) + one, F32),
            pltpu.VMEM((m,) + one, F32),
            pltpu.VMEM(one, F32),
        ]
        + [pltpu.SemaphoreType.DMA((n,))] * 2
        + [pltpu.SemaphoreType.DMA((m,))] * 2,
        compiler_params=pltpu.CompilerParams(collective_id=number, has_side_effects=True),
        name="gain_sum",
    )(cut)


HEAD_DIM = 96


EPS = 1e-05
THETA = 100000.0
NEG = -1e30


def rope_tables(count, width):
    half = width // 2
    freqs = THETA ** (-jnp.arange(half, dtype=jnp.float32) * (2.0 / width))
    angles = jnp.arange(count, dtype=jnp.float32)[:, None] * freqs[None, :]
    return (jnp.cos(angles), jnp.sin(angles))


def rotate(vectors, cosines, sines):
    half = vectors.shape[-1] // 2
    first = vectors[..., :half]
    second = vectors[..., half:]
    cos_b = cosines[:, None, :]
    sin_b = sines[:, None, :]
    return jnp.concatenate(
        [first * cos_b - second * sin_b, second * cos_b + first * sin_b], axis=-1
    )


def unrotate(grads, cosines, sines):
    half = grads.shape[-1] // 2
    first = grads[..., :half]
    second = grads[..., half:]
    cos_b = cosines[:, None, :]
    sin_b = sines[:, None, :]
    return jnp.concatenate(
        [first * cos_b + second * sin_b, second * cos_b - first * sin_b], axis=-1
    )


def transposed(left, right):
    return lax.dot_general(
        left, right, (((1,), (1,)), ((), ())), preferred_element_type=jnp.float32
    )


def outer_sum(left, right):
    return lax.dot_general(
        left, right, (((0,), (0,)), ((), ())), preferred_element_type=jnp.float32
    )


def rms_back(grad_norm, normed, inverse):
    return inverse * (grad_norm - normed * jnp.mean(grad_norm * normed, axis=1, keepdims=True))


def scores_block(query_block, key_prefix, start, seq_positions, key_valid, scale):
    block = query_block.shape[0]
    stop = key_prefix.shape[0]
    raw = (
        jnp.einsum("qcgd,kcd->cgqk", query_block, key_prefix, preferred_element_type=jnp.float32)
        * scale
    )
    rows = start + jnp.arange(block)
    allowed = (seq_positions[None, :stop] <= rows[:, None]) & key_valid[None, :stop]
    return jnp.where(allowed, raw, NEG)


def body(
    activations,
    lengths,
    attn_gain,
    w_query,
    w_key,
    w_value,
    w_out,
    mlp_gain,
    w_gate,
    w_up,
    w_down,
    cotangent,
):
    tensor_size = lax.axis_size("tensor")
    tensor_rank = lax.axis_index("tensor")
    tokens = activations[0].astype(jnp.float32)
    local = tokens.shape[0]
    seq_len = local * tensor_size
    length = lengths[0]
    own_valid = (tensor_rank * local + jnp.arange(local) < length)[:, None]
    seq_positions = jnp.arange(seq_len)
    key_valid = seq_positions < length
    cosines, sines = rope_tables(seq_len, HEAD_DIM)
    scale = 1.0 / math.sqrt(HEAD_DIM)
    q_width, kv_width = w_query.shape[1], w_key.shape[1]
    ff_width = w_gate.shape[1]
    attn_all = lax.all_gather(
        jnp.concatenate([w_query, w_key, w_value, w_out.T], axis=1), "dp", axis=0, tiled=True
    )
    mlp_all = lax.all_gather(
        jnp.concatenate([w_gate, w_up, w_down.T], axis=1), "dp", axis=0, tiled=True
    )
    cuts = (q_width, q_width + kv_width, q_width + 2 * kv_width)
    query_full, key_full, value_full, out_full = jnp.split(attn_all, cuts, axis=1)
    gate_full, up_full, down_full = jnp.split(mlp_all, 3, axis=1)
    gains = gain_gather(0, jnp.stack([attn_gain, mlp_gain]).astype(jnp.float32))
    first_gain_f, second_gain_f = gains[:1], gains[1:]
    heads = q_width // HEAD_DIM
    kv_local = kv_width // HEAD_DIM
    groups = heads // kv_local
    inv_first = lax.rsqrt(jnp.mean(tokens * tokens, axis=1, keepdims=True) + EPS)
    normed_first = tokens * inv_first
    first_low = (normed_first * first_gain_f).astype(jnp.bfloat16)
    (first_all,) = exchange(1, own=first_low)
    query_proj = jnp.dot(first_all, query_full, preferred_element_type=jnp.float32).reshape(
        seq_len, heads, HEAD_DIM
    )
    queries = (
        rotate(query_proj, cosines, sines)
        .astype(jnp.bfloat16)
        .reshape(seq_len, kv_local, groups, HEAD_DIM)
    )
    key_proj = jnp.dot(first_all, key_full, preferred_element_type=jnp.float32).reshape(
        seq_len, kv_local, HEAD_DIM
    )
    keys = rotate(key_proj, cosines, sines).astype(jnp.bfloat16)
    values = (
        jnp.dot(first_all, value_full, preferred_element_type=jnp.float32)
        .astype(jnp.bfloat16)
        .reshape(seq_len, kv_local, HEAD_DIM)
    )
    span = min(512, seq_len)
    count = seq_len // span
    pieces = []
    log_sums = []
    for index in range(count):
        start = index * span
        stop = start + span
        scores = scores_block(
            queries[start:stop], keys[:stop], start, seq_positions, key_valid, scale
        )
        peak = jnp.max(scores, axis=3, keepdims=True)
        log_sum = peak + jnp.log(jnp.sum(jnp.exp(scores - peak), axis=3, keepdims=True))
        probs = jnp.exp(scores - log_sum)
        mixed = jnp.einsum(
            "cgqk,kcd->qcgd",
            probs.astype(jnp.bfloat16),
            values[:stop],
            preferred_element_type=jnp.float32,
        )
        pieces.append(mixed.reshape(span, heads * HEAD_DIM))
        log_sums.append(log_sum)
    attended = jnp.concatenate(pieces, axis=0).astype(jnp.bfloat16)
    grad_result = jnp.where(own_valid, cotangent[0].astype(jnp.float32), 0.0)
    grad_mlp_all, branch = exchange(
        2,
        own=grad_result.astype(jnp.bfloat16),
        part=transposed(attended, out_full).astype(jnp.bfloat16),
    )
    middle = tokens + branch
    inv_second = lax.rsqrt(jnp.mean(middle * middle, axis=1, keepdims=True) + EPS)
    normed_second = middle * inv_second
    second_low = (normed_second * second_gain_f).astype(jnp.bfloat16)
    (second_all,) = exchange(3, own=second_low)
    gate = jnp.dot(second_all, gate_full, preferred_element_type=jnp.float32)
    up_part = jnp.dot(second_all, up_full, preferred_element_type=jnp.float32)
    sigmoid_gate = jax.nn.sigmoid(gate)
    hidden = (gate * sigmoid_gate * up_part).astype(jnp.bfloat16)
    grad_hidden = jnp.dot(grad_mlp_all, down_full, preferred_element_type=jnp.float32)
    grad_gate_low = (
        grad_hidden * up_part * sigmoid_gate * (1.0 + gate * (1.0 - sigmoid_gate))
    ).astype(jnp.bfloat16)
    grad_up_low = (grad_hidden * gate * sigmoid_gate).astype(jnp.bfloat16)
    grad_second_part = (
        transposed(grad_gate_low, gate_full) + transposed(grad_up_low, up_full)
    ).astype(jnp.bfloat16)
    result_part = transposed(hidden, down_full).astype(jnp.bfloat16)
    mlp_grads = lax.psum_scatter(
        jnp.concatenate(
            [
                outer_sum(second_all, grad_gate_low).astype(jnp.bfloat16),
                outer_sum(second_all, grad_up_low).astype(jnp.bfloat16),
                outer_sum(grad_mlp_all, hidden).astype(jnp.bfloat16),
            ],
            axis=1,
        ),
        "dp",
        scatter_dimension=0,
        tiled=True,
    )
    (grad_second,) = exchange(4, part=grad_second_part)
    second_gain_part = jnp.sum(grad_second * normed_second, axis=0)
    grad_middle = grad_result + rms_back(grad_second * second_gain_f, normed_second, inv_second)
    grad_attn_all, result_sum = exchange(
        5, own=grad_middle.astype(jnp.bfloat16), part=result_part
    )
    output = jnp.where(own_valid, middle + result_sum, 0.0)
    grad_attended = jnp.dot(
        grad_attn_all, out_full, preferred_element_type=jnp.float32
    ).astype(jnp.bfloat16)
    out_grads = lax.psum_scatter(
        outer_sum(grad_attn_all, attended).astype(jnp.bfloat16),
        "dp",
        scatter_dimension=0,
        tiled=True,
    )
    grad_queries = []
    grad_keys = jnp.zeros((seq_len, kv_local, HEAD_DIM), jnp.float32)
    grad_values = jnp.zeros((seq_len, kv_local, HEAD_DIM), jnp.float32)
    for index in range(count):
        start = index * span
        stop = start + span
        query_block = queries[start:stop]
        scores = scores_block(query_block, keys[:stop], start, seq_positions, key_valid, scale)
        probs = jnp.exp(scores - log_sums[index])
        grad_block = grad_attended[start:stop].reshape(span, kv_local, groups, HEAD_DIM)
        grad_probs = jnp.einsum(
            "qcgd,kcd->cgqk", grad_block, values[:stop], preferred_element_type=jnp.float32
        )
        row_dot = jnp.sum(probs * grad_probs, axis=3, keepdims=True)
        grad_scores = (probs * (grad_probs - row_dot)).astype(jnp.bfloat16)
        query_grad = (
            jnp.einsum(
                "cgqk,kcd->qcgd", grad_scores, keys[:stop], preferred_element_type=jnp.float32
            )
            * scale
        )
        grad_queries.append(query_grad.reshape(span, heads, HEAD_DIM))
        key_grad = (
            jnp.einsum(
                "cgqk,qcgd->kcd", grad_scores, query_block, preferred_element_type=jnp.float32
            )
            * scale
        )
        grad_keys = grad_keys.at[:stop].add(key_grad)
        value_grad = jnp.einsum(
            "cgqk,qcgd->kcd",
            probs.astype(jnp.bfloat16),
            grad_block,
            preferred_element_type=jnp.float32,
        )
        grad_values = grad_values.at[:stop].add(value_grad)
    grad_query_proj = (
        unrotate(jnp.concatenate(grad_queries, axis=0), cosines, sines)
        .astype(jnp.bfloat16)
        .reshape(seq_len, heads * HEAD_DIM)
    )
    grad_key_proj = (
        unrotate(grad_keys, cosines, sines)
        .astype(jnp.bfloat16)
        .reshape(seq_len, kv_local * HEAD_DIM)
    )
    grad_value_proj = grad_values.astype(jnp.bfloat16).reshape(seq_len, kv_local * HEAD_DIM)
    grad_first_part = (
        transposed(grad_query_proj, query_full)
        + transposed(grad_key_proj, key_full)
        + transposed(grad_value_proj, value_full)
    ).astype(jnp.bfloat16)
    attn_grads = lax.psum_scatter(
        jnp.concatenate(
            [
                outer_sum(first_all, grad_query_proj).astype(jnp.bfloat16),
                outer_sum(first_all, grad_key_proj).astype(jnp.bfloat16),
                outer_sum(first_all, grad_value_proj).astype(jnp.bfloat16),
            ],
            axis=1,
        ),
        "dp",
        scatter_dimension=0,
        tiled=True,
    )
    (grad_first,) = exchange(6, part=grad_first_part)
    first_gain_part = jnp.sum(grad_first * normed_first, axis=0)
    grad_tokens = grad_middle + rms_back(grad_first * first_gain_f, normed_first, inv_first)
    gain_grads = gain_sum(7, jnp.stack([first_gain_part, second_gain_part]))
    grad_query_w, grad_key_w, grad_value_w = jnp.split(
        attn_grads.astype(jnp.float32), cuts[:2], axis=1
    )
    grad_gate_w, grad_up_w, grad_down_w = jnp.split(mlp_grads.astype(jnp.float32), 3, axis=1)
    return (
        output[None],
        grad_tokens[None],
        gain_grads[0],
        grad_query_w,
        grad_key_w,
        grad_value_w,
        out_grads.astype(jnp.float32).T,
        gain_grads[1],
        grad_gate_w,
        grad_up_w,
        grad_down_w.T,
    )


def solution(mesh):
    return jax.shard_map(
        body,
        mesh=mesh,
        in_specs=(
            P("dp", "tensor", None),
            P("dp"),
            P("dp"),
            P("dp", "tensor"),
            P("dp", "tensor"),
            P("dp", "tensor"),
            P("tensor", "dp"),
            P("dp"),
            P("dp", "tensor"),
            P("dp", "tensor"),
            P("tensor", "dp"),
            P("dp", "tensor", None),
        ),
        out_specs=(
            P("dp", "tensor", None),
            P("dp", "tensor", None),
            P("dp"),
            P("dp", "tensor"),
            P("dp", "tensor"),
            P("dp", "tensor"),
            P("tensor", "dp"),
            P("dp"),
            P("dp", "tensor"),
            P("dp", "tensor"),
            P("tensor", "dp"),
        ),
        check_vma=False,
    )
```
